32 devices in a mesh: dp: 2 (over x), col: 4 (over z), row: 4 (over y, core).
Axes of the slice: x: 2, y: 2, z: 4, core: 2. Of those that a mesh axis runs over, the one named last changes fastest.
Arguments:
- hidden: bfloat16 [256, 3584], P('dp', 'row'), parts along dimension 0
- mrope_ids: int32 [3, 256], P(None, ('dp', 'row')), parts along dimension 1
- cache_lens: int32 [256], P(('dp', 'row')), parts along dimension 0
- k_cache: bfloat16 [256, 1024, 4, 128], P(('dp', 'row'), None, 'col'), parts along dimension 0
- v_cache: bfloat16 [256, 1024, 4, 128], P(('dp', 'row'), None, 'col'), parts along dimension 0
- norm_attn: bfloat16 [3584], P('row')
- w_qkv: bfloat16 [3584, 4608], P('row', 'col')
- b_qkv: bfloat16 [4608], P('col')
- w_out: bfloat16 [3584, 3584], P('col', 'row')
- norm_mlp: bfloat16 [3584], P('row')
- w_gate: bfloat16 [3584, 18944], P('row', 'col')
- w_up: bfloat16 [3584, 18944], P('row', 'col')
- w_down: bfloat16 [18944, 3584], P('col', 'row')
Outputs:
- output 1: bfloat16 [256, 3584], P('dp', 'row'), parts along dimension 0
- output 2: bfloat16 [256, 1024, 4, 128], P(('dp', 'row'), None, 'col'), parts along dimension 0
- output 3: bfloat16 [256, 1024, 4, 128], P(('dp', 'row'), None, 'col'), parts along dimension 0
There are 2 independent parts. The reference program is written for one: setup_inputs(seed, part) draws one part's arguments, and reference() takes and returns one part's arrays. A program takes and returns all parts, laid end to end along the dimension named above; an argument that names none is the same for every part.
All inputs are finite; a program needn't handle non-finite values.
Results may differ from the reference program's by a relative error of at most 0.0153839.
Values are sent between devices in bfloat16 or wider.
A program may use at most 1 GiB of HBM per device.

```python
import math
import jax
import jax.numpy as jnp
from jax import lax

D = 3584
HEADS = 28
KV_HEADS = 4
FF = 18944
HEAD_DIM = 128
CACHE_LEN = 1024
BATCH = 128

GROUP = HEADS // KV_HEADS
QKV_COLS = (HEADS + 2 * KV_HEADS) * HEAD_DIM
ATTN_COLS = HEADS * HEAD_DIM
ROPE_THETA = 1000000.0
NORM_EPS = 1e-6
K_SCALE = math.sqrt(math.log(CACHE_LEN) / 3.0)


def draw_positions(key):
    sub_keys = jax.random.split(key, 6)
    seq_lens = jax.random.randint(sub_keys[0], (BATCH,), CACHE_LEN // 16, CACHE_LEN)
    top_row = jax.random.randint(sub_keys[1], (), 0, BATCH)
    seq_lens = jnp.where(jnp.arange(BATCH) == top_row, CACHE_LEN - 1, seq_lens)
    after_image = jax.random.randint(sub_keys[2], (BATCH,), 0, 2) == 1
    text_ids = jax.random.randint(sub_keys[3], (BATCH,), seq_lens // 2, seq_lens + 1)
    image_ids = jax.random.randint(sub_keys[4], (BATCH,), 0, seq_lens // 2 + 1)
    offsets = jax.random.randint(sub_keys[5], (2, BATCH), 1, 48)
    mrope_ids = jnp.stack([
        jnp.where(after_image, image_ids, text_ids),
        jnp.where(after_image, image_ids + offsets[0], text_ids),
        jnp.where(after_image, image_ids + offsets[1], text_ids)])
    return mrope_ids.astype(jnp.int32), seq_lens.astype(jnp.int32)


def normal_draw(key, shape, scale):
    return (jax.random.normal(key, shape, jnp.float32) * scale).astype(jnp.bfloat16)


def setup_inputs(seed: int = 0, part: int = 0) -> dict:
    shared_keys = jax.random.split(jax.random.key(seed), 8)
    own_keys = jax.random.split(jax.random.fold_in(jax.random.key(seed + 1), part), 4)
    mrope_ids, cache_lens = draw_positions(own_keys[3])
    cache_shape = (BATCH, CACHE_LEN, KV_HEADS, HEAD_DIM)
    return dict(
        hidden=normal_draw(own_keys[0], (BATCH, D), 1.0),
        mrope_ids=mrope_ids,
        cache_lens=cache_lens,
        k_cache=normal_draw(own_keys[1], cache_shape, K_SCALE),
        v_cache=normal_draw(own_keys[2], cache_shape, 1.0),
        norm_attn=(1.0 + 0.3 * jax.random.normal(shared_keys[0], (D,), jnp.float32)).astype(jnp.bfloat16),
        w_qkv=normal_draw(shared_keys[1], (D, QKV_COLS), D ** -0.5),
        b_qkv=normal_draw(shared_keys[2], (QKV_COLS,), 0.5),
        w_out=normal_draw(shared_keys[3], (ATTN_COLS, D), ATTN_COLS ** -0.5),
        norm_mlp=(1.0 + 0.3 * jax.random.normal(shared_keys[4], (D,), jnp.float32)).astype(jnp.bfloat16),
        w_gate=normal_draw(shared_keys[5], (D, FF), D ** -0.5),
        w_up=normal_draw(shared_keys[6], (D, FF), D ** -0.5),
        w_down=normal_draw(shared_keys[7], (FF, D), FF ** -0.5))


def rms_norm(values, gain):
    hid_f = values.astype(jnp.float32)
    mean_sq = jnp.mean(hid_f * hid_f, axis=-1, keepdims=True)
    return (hid_f * lax.rsqrt(mean_sq + NORM_EPS) * gain.astype(jnp.float32)).astype(jnp.bfloat16)


def rope_tables(mrope_ids):
    pair = jnp.arange(HEAD_DIM // 2)
    inv_freq = 1.0 / (ROPE_THETA ** (pair.astype(jnp.float32) * 2.0 / HEAD_DIM))
    pos_f = mrope_ids.astype(jnp.float32)
    chosen = jnp.where(pair[None, :] < 16, pos_f[0][:, None],
                       jnp.where(pair[None, :] < 40, pos_f[1][:, None], pos_f[2][:, None]))
    angles = chosen * inv_freq[None, :]
    return jnp.cos(angles), jnp.sin(angles)


def apply_rope(vec, cos_t, sin_t):
    vec_f = vec.astype(jnp.float32)
    half = HEAD_DIM // 2
    lower = vec_f[..., :half]
    upper = vec_f[..., half:]
    return jnp.concatenate([lower * cos_t - upper * sin_t, upper * cos_t + lower * sin_t], axis=-1).astype(jnp.bfloat16)


def attend_row(row_args):
    q_row, k_row, v_row, row_len = row_args
    positions = jnp.arange(CACHE_LEN)
    scores = jnp.einsum('hgd,lhd->hgl', q_row.astype(jnp.float32), k_row.astype(jnp.float32)) * (HEAD_DIM ** -0.5)
    scores = jnp.where(positions[None, None, :] <= row_len, scores, -1e30)
    attn_prob = jax.nn.softmax(scores, axis=-1).astype(jnp.bfloat16)
    return jnp.einsum('hgl,lhd->hgd', attn_prob.astype(jnp.float32), v_row.astype(jnp.float32)).astype(jnp.bfloat16)


def reference(hidden, mrope_ids, cache_lens, k_cache, v_cache, norm_attn, w_qkv, b_qkv, w_out, norm_mlp, w_gate, w_up, w_down):
    normed = rms_norm(hidden, norm_attn)
    qkv_rows = (jnp.dot(normed, w_qkv, preferred_element_type=jnp.float32) + b_qkv.astype(jnp.float32)).astype(jnp.bfloat16)
    qkv_rows = qkv_rows.reshape(BATCH, KV_HEADS, GROUP + 2, HEAD_DIM)
    cos_t, sin_t = rope_tables(mrope_ids)
    query = apply_rope(qkv_rows[:, :, :GROUP], cos_t[:, None, None], sin_t[:, None, None])
    new_key = apply_rope(qkv_rows[:, :, GROUP], cos_t[:, None], sin_t[:, None])
    new_val = qkv_rows[:, :, GROUP + 1]
    slot_hit = jnp.arange(CACHE_LEN)[None, :, None, None] == cache_lens[:, None, None, None]
    k_next = jnp.where(slot_hit, new_key[:, None], k_cache)
    v_next = jnp.where(slot_hit, new_val[:, None], v_cache)
    attn = lax.map(attend_row, (query, k_next, v_next, cache_lens))
    attn_proj = jnp.dot(attn.reshape(BATCH, ATTN_COLS), w_out, preferred_element_type=jnp.float32)
    resid_mid = (hidden.astype(jnp.float32) + attn_proj).astype(jnp.bfloat16)
    normed_mlp = rms_norm(resid_mid, norm_mlp)
    gate_proj = jnp.dot(normed_mlp, w_gate, preferred_element_type=jnp.float32).astype(jnp.bfloat16)
    up_proj = jnp.dot(normed_mlp, w_up, preferred_element_type=jnp.float32).astype(jnp.bfloat16)
    mlp_act = (jax.nn.silu(gate_proj.astype(jnp.float32)) * up_proj.astype(jnp.float32)).astype(jnp.bfloat16)
    down_proj = jnp.dot(mlp_act, w_down, preferred_element_type=jnp.float32)
    hidden_out = (resid_mid.astype(jnp.float32) + down_proj).astype(jnp.bfloat16)
    return (hidden_out, k_next, v_next)
```

```python
import functools

import jax
import jax.numpy as jnp
import numpy as np
from jax import lax
from jax.experimental import pallas as pl
from jax.experimental.pallas import tpu as pltpu
from jax.sharding import PartitionSpec as P

MESH = pl.DeviceIdType.MESH
LANES = 128
HEAD_DIM = 128
ROPE_THETA = 1000000.0
NORM_EPS = 1e-6
DOWNSCALE = 2.0 ** -10
BIG = 3.3e38
GROUPS = 2
UNROLL = 8
CACHE_PARTS = 8
CHUNKS = (4, 8, 8, 8, 6, 3)
EARLY = 3
SPREAD_AT = 3
F32 = jnp.float32
BF16 = jnp.bfloat16


def row_peers():
    row = lax.axis_index('row')
    core, y = row % 2, row // 2
    return row, y * 2 + 1 - core, (1 - y) * 2 + core, (1 - y) * 2 + 1 - core


def split_square(sq_sum):
    high = sq_sum.astype(BF16)
    high_f = high.astype(F32)
    low = jnp.where(high_f < BIG, sq_sum - high_f, 0.0).astype(BF16)
    return high, low


def local_scale(sq_sum, width):
    return lax.rsqrt(sq_sum / width + NORM_EPS)


def ratio(total, local):
    return jnp.where(local > 0.0, total / local, 0.0)


def remote(src, dst, send_sem, recv_sem, device):
    return pltpu.make_async_remote_copy(src_ref=src, dst_ref=dst, send_sem=send_sem, recv_sem=recv_sem,
                                        device_id=device, device_id_type=MESH)


def rotate(vec, cos_t, sin_t):
    half = HEAD_DIM // 2
    swapped = jnp.concatenate([-vec[:, half:], vec[:, :half]], axis=1)
    return (vec * cos_t + swapped * sin_t).astype(BF16).astype(F32)


def qkv_kernel(h_hbm, g_hbm, w_hbm, b_hbm, ids_hbm, freq_hbm, kc_hbm, vc_hbm, q_ref, k_ref, v_ref, kc_ref, vc_ref,
               h_ref, g_ref, w_ref, b_ref, ids_ref, freq_ref, part, send, recv, table, q_rows,
               send_sem, recv_sem, load_sem, cache_sem):
    row, *peers = row_peers()
    loads = [pltpu.make_async_copy(src, dst, load_sem.at[i]) for i, (src, dst) in enumerate(
        ((h_hbm, h_ref), (g_hbm, g_ref), (w_hbm, w_ref), (b_hbm, b_ref), (ids_hbm, ids_ref), (freq_hbm, freq_ref)))]
    for copy in loads:
        copy.start()
    width = h_ref.shape[1]
    cols = w_ref.shape[1]
    rows = k_ref.shape[0]
    group = cols // HEAD_DIM - 2
    barrier = pltpu.get_barrier_semaphore()
    for peer in peers:
        pl.semaphore_signal(barrier, inc=1, device_id={'row': peer}, device_id_type=MESH)
    cache_copies = []
    for i in range(CACHE_PARTS):
        at = pl.ds(i * (rows // CACHE_PARTS), rows // CACHE_PARTS)
        cache_copies.append(pltpu.make_async_copy(kc_hbm.at[at], kc_ref.at[at], cache_sem.at[0, i]))
        cache_copies.append(pltpu.make_async_copy(vc_hbm.at[at], vc_ref.at[at], cache_sem.at[1, i]))
    for copy in cache_copies:
        copy.start()

    loads[0].wait()
    loads[1].wait()
    hid = h_ref[...].astype(F32)
    sq_sum = jnp.sum(hid * hid, axis=1, keepdims=True)
    scale = local_scale(sq_sum, width) * DOWNSCALE
    normed = (hid * scale * g_ref[...].astype(F32).reshape(1, -1)).astype(BF16)
    loads[2].wait()
    prod = jnp.dot(normed, w_ref[...], preferred_element_type=F32)
    part[:, 0:cols] = prod
    wide = jnp.broadcast_to(sq_sum, (hid.shape[0], LANES))
    part[:, cols:] = wide
    send[:, 0:cols] = prod.astype(BF16)
    high, low = split_square(wide)
    send[:, cols:cols + LANES] = high
    send[:, cols + LANES:] = low
    pl.semaphore_wait(barrier, 3)
    copies = []
    for slot in (2, 1, 0):
        copies.append(remote(send.at[pl.ds(pl.multiple_of(peers[slot] * rows, rows), rows)], recv.at[slot],
                             send_sem.at[slot], recv_sem.at[slot], {'row': peers[slot]}))
        copies[-1].start()

    for copy in loads[3:]:
        copy.wait()
    table[...] = jnp.zeros_like(table)
    table[0:3, 0:rows] = ids_ref[...].astype(F32)
    by_row = table[...].T
    pair = lax.broadcasted_iota(jnp.int32, (rows, HEAD_DIM), 1) % (HEAD_DIM // 2)
    chosen = jnp.where(pair < 16, by_row[0:rows, 0:1], jnp.where(pair < 40, by_row[0:rows, 1:2], by_row[0:rows, 2:3]))
    angles = chosen * freq_ref[...]
    cos_t, sin_t = jnp.cos(angles), jnp.sin(angles)

    for copy in copies:
        copy.wait_recv()
    mine = part[pl.ds(pl.multiple_of(row * rows, rows), rows), :]
    sums = [mine[:, cols:cols + 1]]
    parts = [mine[:, 0:cols]]
    for slot in range(3):
        block = recv[slot].astype(F32)
        sums.append(block[:, cols:cols + 1] + block[:, cols + LANES:cols + LANES + 1])
        parts.append(block[:, 0:cols])
    total = local_scale(sums[0] + sums[1] + sums[2] + sums[3], 4 * width)
    qkv = jnp.zeros((rows, cols), F32)
    for square, block in zip(sums, parts):
        qkv = qkv + block * ratio(total, local_scale(square, width) * DOWNSCALE)
    qkv = (qkv + b_ref[...].astype(F32).reshape(1, -1)).astype(BF16).astype(F32)
    for head in range(group):
        q_rows[pl.ds(head, rows, stride=8), :] = rotate(qkv[:, head * HEAD_DIM:(head + 1) * HEAD_DIM], cos_t, sin_t)
    for head in range(group, 8):
        q_rows[pl.ds(head, rows, stride=8), :] = jnp.zeros((rows, HEAD_DIM), F32)
    q_ref[...] = q_rows[...]
    k_ref[...] = rotate(qkv[:, group * HEAD_DIM:(group + 1) * HEAD_DIM], cos_t, sin_t)
    v_ref[...] = qkv[:, (group + 1) * HEAD_DIM:]
    for copy in copies:
        copy.wait_send()
    for copy in cache_copies:
        copy.wait()


def attention_kernel(group, unroll, lens_ref, q_ref, nk_ref, nv_ref, k_ref, v_ref, o_ref, k_out, v_out,
                     k_patch, v_patch, o_rows, s_buf, out_sem, patch_sem):
    rows, slots = k_ref.shape[0], k_ref.shape[1]
    steps = rows // unroll

    def stores(step):
        at = pl.ds(step * unroll, unroll)
        return (pltpu.make_async_copy(k_ref.at[at], k_out.at[at], out_sem.at[0, step]),
                pltpu.make_async_copy(v_ref.at[at], v_out.at[at], out_sem.at[1, step]))

    def patches(b):
        base = pl.multiple_of((lens_ref[b] // 16) * 16, 16)
        return (pltpu.make_async_copy(k_patch.at[b], k_out.at[b, pl.ds(base, 16)], patch_sem.at[0, b]),
                pltpu.make_async_copy(v_patch.at[b], v_out.at[b, pl.ds(base, 16)], patch_sem.at[1, b]))

    for step in range(steps):
        for copy in stores(step):
            copy.start()

    @pl.loop(0, rows)
    def _(b):
        base = pl.multiple_of((lens_ref[b] // 16) * 16, 16)
        hit = lax.broadcasted_iota(jnp.int32, (16, HEAD_DIM), 0) == lens_ref[b] % 16
        for src, new, patch in ((k_ref, nk_ref, k_patch), (v_ref, nv_ref, v_patch)):
            old = src[b, pl.ds(base, 16), :].astype(F32)
            patch[b] = jnp.where(hit, new[pl.ds(b, 1), :], old).astype(BF16)

    @pl.loop(0, steps)
    def _(step):
        items = [step * unroll + u for u in range(unroll)]
        position = lax.broadcasted_iota(jnp.int32, (8, slots), 1)
        for u, b in enumerate(items):
            query = q_ref[pl.ds(pl.multiple_of(b * 8, 8), 8), :]
            scores = lax.dot_general(query.astype(BF16), k_ref[b], (((1,), (1,)), ((), ())), preferred_element_type=F32)
            fresh = jnp.sum(query * nk_ref[pl.ds(b, 1), :], axis=1, keepdims=True)
            scores = jnp.where(position == lens_ref[b], fresh, scores) * (HEAD_DIM ** -0.5)
            s_buf[u * 8:(u + 1) * 8, :] = jnp.where(position <= lens_ref[b], scores, -1e30)
        scores = s_buf[...]
        weight = jnp.exp(scores - jnp.max(scores, axis=1, keepdims=True))
        s_buf[...] = weight / jnp.sum(weight, axis=1, keepdims=True)
        for u, b in enumerate(items):
            prob = s_buf[u * 8:(u + 1) * 8, :].astype(BF16)
            newest = position == lens_ref[b]
            prob_f = prob.astype(F32)
            fresh = jnp.sum(jnp.where(newest, prob_f, 0.0), axis=1, keepdims=True)
            rest = jnp.where(newest, 0.0, prob_f).astype(BF16)
            o_rows[pl.ds(pl.multiple_of(b * 8, 8), 8), :] = (
                jnp.dot(rest, v_ref[b], preferred_element_type=F32) + fresh * nv_ref[pl.ds(b, 1), :])

    for head in range(group):
        o_ref[:, head * HEAD_DIM:(head + 1) * HEAD_DIM] = o_rows[pl.ds(head, rows, stride=8), :].astype(BF16)

    for step in range(steps):
        for copy in stores(step):
            copy.wait()

        @pl.loop(step * unroll, (step + 1) * unroll)
        def _(b):
            for copy in patches(b):
                copy.start()

    @pl.loop(0, rows)
    def _(b):
        for copy in patches(b):
            copy.wait()


def mlp_kernel(chunks, o_ref, h_hbm, g_hbm, wo_hbm, wg_hbm, wu_hbm, wd_hbm, out_ref,
               hid, g_ref, wo, wgu, wd, o_all, osend, orecv, own, resid, resid_p, z_p, sums_p, coef,
               part, send1, recv1, send2, recv2, acts, acc, dsend, drecv, final,
               h_sem, g_sem, wo_sem, wgu_sem, wd_sem, osem, rs_sem, ag_sem, s1_sem, s2_sem, ay_sem, ac_sem, aw_sem, ds_sem, da_sem):
    row, mate, across, diagonal = row_peers()
    core, y = row % 2, row // 2
    col = lax.axis_index('col')
    zpeers = [(col + step) % 4 for step in (1, 2, 3)]
    n_tiles = wgu.shape[0]
    width = hid.shape[1]
    group_rows = resid.shape[1]
    rows = group_rows // 2
    block = group_rows // 4
    base = [pl.multiple_of(y * group_rows, group_rows), pl.multiple_of((1 - y) * group_rows, group_rows)]
    n_chunks = len(chunks)
    last = n_chunks - 1

    mine = pl.ds(pl.multiple_of(core * rows, rows), rows)
    theirs = pl.ds(pl.multiple_of((1 - core) * rows, rows), rows)
    wo_copy = pltpu.make_async_copy(wo_hbm, wo, wo_sem)
    wo_copy.start()
    h_copy = pltpu.make_async_copy(h_hbm, hid, h_sem)
    h_copy.start()
    g_copy = pltpu.make_async_copy(g_hbm, g_ref, g_sem)
    g_copy.start()

    barrier = pltpu.get_barrier_semaphore()
    for peer in (diagonal, across, mate):
        pl.semaphore_signal(barrier, inc=1, device_id={'row': peer}, device_id_type=MESH)
    for peer in zpeers:
        pl.semaphore_signal(barrier, inc=1, device_id={'col': peer}, device_id_type=MESH)

    def tile_loads(t):
        at = pl.ds(pl.multiple_of(t * LANES, LANES), LANES)
        return (pltpu.make_async_copy(wg_hbm.at[:, at], wgu.at[t, :, pl.ds(0, LANES)], wgu_sem.at[0, t]),
                pltpu.make_async_copy(wu_hbm.at[:, at], wgu.at[t, :, pl.ds(LANES, LANES)], wgu_sem.at[1, t]))

    @pl.loop(0, n_tiles)
    def _(t):
        for copy in tile_loads(t):
            copy.start()

    wd_copies = []
    for k, (first, count) in enumerate(chunks):
        at = pl.ds(first * LANES, count * LANES)
        wd_copies.append(pltpu.make_async_copy(wd_hbm.at[at], wd.at[at], wd_sem.at[k]))
        wd_copies[-1].start()

    started = []

    def start(copy):
        copy.start()
        started.append(copy)
        return copy

    o_all[0, mine, :] = o_ref[...]
    pl.semaphore_wait(barrier, 6)
    gathers = [start(remote(o_ref, o_all.at[g, mine], osem.at[0, i], osem.at[1, i], {'row': peer}))
               for i, g, peer in ((0, 0, mate), (1, 1, across), (2, 1, diagonal))]

    own_rows = pl.ds(pl.multiple_of(col * block, block), block)
    scatters, spreads = {}, {}

    def project(g):
        if g == 0:
            wo_copy.wait()
            gathers[0].wait_recv()
        else:
            gathers[1].wait_recv()
            gathers[2].wait_recv()
        prod = jnp.dot(o_all[g], wo[...], preferred_element_type=F32)
        own[g] = prod
        osend[g] = prod.astype(BF16)
        scatters[g] = [start(remote(osend.at[g, pl.ds(pl.multiple_of(zpeers[i] * block, block), block)], orecv.at[g, i],
                                    rs_sem.at[0, g, i], rs_sem.at[1, g, i], {'col': zpeers[i]})) for i in (1, 2, 0)]

    def spread(g):
        if g == 0:
            h_copy.wait()
            g_copy.wait()
        for copy in scatters[g]:
            copy.wait_recv()
        total = own[g, own_rows, :]
        for i in range(3):
            total = total + orecv[g, i].astype(F32)
        old = hid[pl.ds(pl.multiple_of(base[g] + col * block, block), block), :].astype(F32)
        resid[g, own_rows, :] = (old + total).astype(BF16)
        spreads[g] = [start(remote(resid.at[g, own_rows], resid.at[g, own_rows], ag_sem.at[0, g, i], ag_sem.at[1, g, i],
                                   {'col': zpeers[i]})) for i in (1, 2, 0)]

    stage1, stage2, act_y, act_c, act_w = {}, {}, {}, {}, {}

    def norm(g):
        for copy in spreads[g]:
            copy.wait_recv()
        resid_p[g, 0:rows, :] = resid[g, mine, :]
        resid_p[g, rows:, :] = resid[g, theirs, :]
        res = resid_p[g].astype(F32)
        sq_sum = jnp.sum(res * res, axis=1, keepdims=True)
        z_p[g] = (res * (local_scale(sq_sum, width) * DOWNSCALE) * g_ref[...].astype(F32).reshape(1, -1)).astype(BF16)
        wide = jnp.broadcast_to(sq_sum, (group_rows, LANES))
        sums_p[g] = wide[0:rows]
        high, low = split_square(wide[rows:])
        send1[g, n_tiles, :, 0:LANES] = high
        send1[g, n_tiles, :, LANES:] = low
        stage1[g, n_chunks] = start(remote(send1.at[g, n_tiles], recv1.at[g, n_tiles], s1_sem.at[0, g, n_chunks],
                                           s1_sem.at[1, g, n_chunks], {'row': mate}))

    def multiply(g, k):
        first, count = chunks[k]
        if g == 0:
            @pl.loop(first, first + count)
            def _(t):
                for copy in tile_loads(t):
                    copy.wait()

        @pl.loop(first, first + count, unroll=count)
        def _(t):
            prod = jnp.dot(z_p[g], wgu[t], preferred_element_type=F32)
            part[g, t] = prod[0:rows]
            send1[g, t] = prod[rows:].astype(BF16)

        at = pl.ds(first, count)
        stage1[g, k] = start(remote(send1.at[g, at], recv1.at[g, at], s1_sem.at[0, g, k], s1_sem.at[1, g, k],
                                    {'row': mate}))

    def combine(g, k):
        first, count = chunks[k]
        if k == 0:
            stage1[g, n_chunks].wait_recv()
            got = recv1[g, n_tiles].astype(F32)
            got = got[:, 0:LANES] + got[:, LANES:]
            mine_sq = sums_p[g]
            chip_sq = mine_sq + got
            chip = local_scale(chip_sq, 2 * width)
            mine_c = ratio(chip, local_scale(mine_sq, width) * DOWNSCALE)
            mate_c = ratio(chip, local_scale(got, width) * DOWNSCALE)
            for lane in range(2):
                coef[g, 0, :, lane * LANES:(lane + 1) * LANES] = mine_c
                coef[g, 1, :, lane * LANES:(lane + 1) * LANES] = mate_c
            sums_p[g] = chip_sq
            if g == 0:
                high, low = split_square(chip_sq)
                send2[n_tiles, :, 0:LANES] = high
                send2[n_tiles, :, LANES:] = low
                stage2[n_chunks] = start(remote(send2.at[n_tiles], recv2.at[n_tiles], s2_sem.at[0, n_chunks],
                                                s2_sem.at[1, n_chunks], {'row': across}))
        stage1[g, k].wait_recv()

        @pl.loop(first, first + count, unroll=2 if count % 2 == 0 else 1)
        def _(t):
            chip = part[g, t] * coef[g, 0] + recv1[g, t].astype(F32) * coef[g, 1]
            if g == 0:
                send2[t] = chip.astype(BF16)
            else:
                part[g, t] = chip

        if g == 0:
            at = pl.ds(first, count)
            stage2[k] = start(remote(send2.at[at], recv2.at[at], s2_sem.at[0, k], s2_sem.at[1, k], {'row': across}))

    def activate(k):
        first, count = chunks[k]
        if k == 0:
            stage2[n_chunks].wait_recv()
            got = recv2[n_tiles].astype(F32)
            got = got[:, 0:LANES] + got[:, LANES:]
            chip_sq = sums_p[1]
            total = local_scale(chip_sq + got, 4 * width)
            mine_c = ratio(total, local_scale(chip_sq, 2 * width))
            other_c = ratio(total, local_scale(got, 2 * width))
            for lane in range(2):
                coef[2, 0, :, lane * LANES:(lane + 1) * LANES] = mine_c
                coef[2, 1, :, lane * LANES:(lane + 1) * LANES] = other_c
        stage2[k].wait_recv()

        @pl.loop(first, first + count, unroll=2 if count % 2 == 0 else 1)
        def _(t):
            full = part[1, t] * coef[2, 0] + recv2[t].astype(F32) * coef[2, 1]
            full = full.astype(BF16).astype(F32)
            gate, up = full[:, 0:LANES], full[:, LANES:]
            acts[1, 0:rows, pl.ds(pl.multiple_of(t * LANES, LANES), LANES)] = (
                gate * (1.0 / (1.0 + jnp.exp(-gate))) * up).astype(BF16)

        at = pl.ds(first * LANES, count * LANES)
        src = acts.at[1, pl.ds(0, rows), at]
        act_y[k] = start(remote(src, acts.at[0, pl.ds(0, rows), at], ay_sem.at[0, k], ay_sem.at[1, k], {'row': across}))
        act_c[k] = start(remote(src, acts.at[1, pl.ds(rows, rows), at], ac_sem.at[0, k], ac_sem.at[1, k], {'row': mate}))

    def relay(k):
        first, count = chunks[k]
        at = pl.ds(first * LANES, count * LANES)
        act_y[k].wait_recv()
        act_w[k] = start(remote(acts.at[0, pl.ds(0, rows), at], acts.at[0, pl.ds(rows, rows), at],
                                aw_sem.at[0, k], aw_sem.at[1, k], {'row': mate}))

    def down(g, k):
        first, count = chunks[k]
        if g == 1:
            act_c[k].wait_recv()
            wd_copies[k].wait()
        else:
            act_w[k].wait_recv()
        at = pl.ds(first * LANES, count * LANES)
        prod = jnp.dot(acts[g, :, at], wd[at, :], preferred_element_type=F32)
        acc[g] = prod if k == 0 else acc[g] + prod

    down_scatter, down_spread = {}, {}

    def scatter_down(g):
        dsend[g] = acc[g].astype(BF16)
        down_scatter[g] = [start(remote(dsend.at[g, pl.ds(pl.multiple_of(zpeers[i] * block, block), block)],
                                        drecv.at[g, i], ds_sem.at[0, g, i], ds_sem.at[1, g, i], {'col': zpeers[i]}))
                           for i in (1, 2, 0)]

    def spread_down(g):
        for copy in down_scatter[g]:
            copy.wait_recv()
        total = acc[g, own_rows, :] + resid_p[g, own_rows, :].astype(F32)
        for i in range(3):
            total = total + drecv[g, i].astype(F32)
        final[g, own_rows, :] = total.astype(BF16)
        down_spread[g] = [start(remote(final.at[g, own_rows], final.at[g, own_rows], da_sem.at[0, g, i],
                                       da_sem.at[1, g, i], {'col': zpeers[i]})) for i in (1, 2, 0)]

    def finish(g):
        for copy in down_spread[g]:
            copy.wait_recv()
        for i, half in enumerate((core, 1 - core)):
            out_ref[pl.ds(pl.multiple_of(base[g] + half * rows, rows), rows), :] = final[g, i * rows:(i + 1) * rows, :]

    plan = [(project, 0), (project, 1), (spread, 0), (spread, 1), (norm, 0)]
    for k in range(n_chunks):
        plan += [(multiply, 0, k)] + ([(combine, 0, k - 1)] if k else [])
    plan += [(combine, 0, last), (norm, 1)]
    for k in range(n_chunks):
        plan += [(multiply, 1, k)] + ([(combine, 1, k - 1)] if k else [])
        if k >= EARLY:
            plan += [(activate, k - EARLY)]
    plan += [(combine, 1, last)]
    done = 0
    for k in range(n_chunks - EARLY, n_chunks):
        plan += [(activate, k)]
        while done < k:
            plan += [(down, 1, done)]
            done += 1
    plan += [(down, 1, last), (scatter_down, 1)]
    for k in range(n_chunks):
        plan += [(relay, k)] + ([(down, 0, k - 1)] if k else [])
        if k == SPREAD_AT:
            plan += [(spread_down, 1)]
    plan += [(down, 0, last), (scatter_down, 0), (finish, 1), (spread_down, 0), (finish, 0)]
    for step, *where in plan:
        step(*where)
    for copy in started:
        copy.wait_send()


def solution(mesh):
    cache_spec = P(('dp', 'row'), None, 'col', None)
    in_specs = (P('dp', 'row'), P(None, ('dp', 'row')), P(('dp', 'row')), cache_spec, cache_spec,
                P('row'), P('row', 'col'), P('col'), P('col', 'row'), P('row'),
                P('row', 'col'), P('row', 'col'), P('col', 'row'))
    out_specs = (P('dp', 'row'), cache_spec, cache_spec)
    vmem = pl.BlockSpec(memory_space=pltpu.VMEM)
    smem = pl.BlockSpec(memory_space=pltpu.SMEM)
    hbm = pl.BlockSpec(memory_space=pl.ANY)
    dma = pltpu.SemaphoreType.DMA
    pair = np.arange(HEAD_DIM) % (HEAD_DIM // 2)
    freq = (1.0 / (ROPE_THETA ** (pair.astype(np.float64) * 2.0 / HEAD_DIM))).astype(np.float32)[None, :]

    def local_layer(hidden, mrope_ids, cache_lens, k_cache, v_cache, norm_attn, w_qkv, b_qkv, w_out, norm_mlp, w_gate, w_up, w_down):
        batch, width = hidden.shape
        rows, slots, _, _ = k_cache.shape
        cols = w_qkv.shape[1]
        ff = w_gate.shape[1]
        heads = cols // HEAD_DIM - 2
        (k_flat, v_flat, hidden, w_qkv, w_out, w_gate, w_up, w_down, norm_attn, b_qkv, mrope_ids, norm_mlp, freqs) = (
            pltpu.with_memory_space_constraint(value, pltpu.HBM)
            for value in (k_cache.reshape(rows, slots, HEAD_DIM), v_cache.reshape(rows, slots, HEAD_DIM),
                          hidden, w_qkv, w_out, w_gate, w_up, w_down, norm_attn, b_qkv, mrope_ids, norm_mlp, jnp.asarray(freq)))
        cache_shape = (rows, slots, HEAD_DIM)
        query, new_key, new_val, k_near, v_near = pl.pallas_call(
            qkv_kernel, name='qkv',
            out_shape=(pltpu.VMEM((rows * 8, HEAD_DIM), F32), pltpu.VMEM((rows, HEAD_DIM), F32), pltpu.VMEM((rows, HEAD_DIM), F32),
                       pltpu.VMEM(cache_shape, BF16), pltpu.VMEM(cache_shape, BF16)),
            in_specs=[hbm] * 8, out_specs=(vmem,) * 5,
            scratch_shapes=[pltpu.VMEM((batch, width), BF16), pltpu.VMEM(norm_attn.shape, BF16), pltpu.VMEM(w_qkv.shape, BF16),
                            pltpu.VMEM(b_qkv.shape, BF16), pltpu.VMEM(mrope_ids.shape, jnp.int32), pltpu.VMEM(freq.shape, F32),
                            pltpu.VMEM((batch, cols + LANES), F32), pltpu.VMEM((batch, cols + 2 * LANES), BF16),
                            pltpu.VMEM((3, rows, cols + 2 * LANES), BF16), pltpu.VMEM((LANES, LANES), F32),
                            pltpu.VMEM((rows * 8, HEAD_DIM), F32), dma((3,)), dma((3,)), dma((6,)), dma((2, CACHE_PARTS))],
            compiler_params=pltpu.CompilerParams(collective_id=0, has_side_effects=True, vmem_limit_bytes=12 << 20),
        )(hidden, norm_attn, w_qkv, b_qkv, mrope_ids, freqs, k_flat, v_flat)

        attn, k_next, v_next = pl.pallas_call(
            functools.partial(attention_kernel, heads, UNROLL), name='attend',
            out_shape=(pltpu.VMEM((rows, heads * HEAD_DIM), BF16),
                       jax.ShapeDtypeStruct(cache_shape, BF16), jax.ShapeDtypeStruct(cache_shape, BF16)),
            in_specs=[smem, vmem, vmem, vmem, vmem, vmem], out_specs=(vmem, hbm, hbm),
            scratch_shapes=[pltpu.VMEM((rows, 16, HEAD_DIM), BF16), pltpu.VMEM((rows, 16, HEAD_DIM), BF16),
                            pltpu.VMEM((rows * 8, HEAD_DIM), F32), pltpu.VMEM((UNROLL * 8, slots), F32),
                            dma((2, rows // UNROLL)), dma((2, rows))],
            compiler_params=pltpu.CompilerParams(vmem_limit_bytes=8 << 20),
        )(cache_lens, query, new_key, new_val, k_near, v_near)

        n_tiles = ff // LANES
        chunks = [(sum(CHUNKS[:i]), count) for i, count in enumerate(CHUNKS)]
        n_chunks = len(chunks)
        gr = batch // GROUPS
        half, block = gr // 2, gr // 4
        hidden_out = pl.pallas_call(
            functools.partial(mlp_kernel, chunks), name='mlp',
            out_shape=pltpu.VMEM((batch, width), BF16),
            in_specs=[vmem] + [hbm] * 6, out_specs=vmem,
            scratch_shapes=[
                pltpu.VMEM((batch, width), BF16), pltpu.VMEM(norm_mlp.shape, BF16),
                pltpu.VMEM(w_out.shape, BF16), pltpu.VMEM((n_tiles, width, 2 * LANES), BF16), pltpu.VMEM(w_down.shape, BF16),
                pltpu.VMEM((GROUPS, gr, w_out.shape[0]), BF16), pltpu.VMEM((GROUPS, gr, width), BF16),
                pltpu.VMEM((GROUPS, 3, block, width), BF16), pltpu.VMEM((GROUPS, gr, width), F32),
                pltpu.VMEM((GROUPS, gr, width), BF16), pltpu.VMEM((GROUPS, gr, width), BF16),
                pltpu.VMEM((GROUPS, gr, width), BF16), pltpu.VMEM((GROUPS, half, LANES), F32),
                pltpu.VMEM((GROUPS + 1, 2, half, 2 * LANES), F32),
                pltpu.VMEM((GROUPS, n_tiles, half, 2 * LANES), F32),
                pltpu.VMEM((GROUPS, n_tiles + 1, half, 2 * LANES), BF16),
                pltpu.VMEM((GROUPS, n_tiles + 1, half, 2 * LANES), BF16),
                pltpu.VMEM((n_tiles + 1, half, 2 * LANES), BF16), pltpu.VMEM((n_tiles + 1, half, 2 * LANES), BF16),
                pltpu.VMEM((GROUPS, gr, ff), BF16), pltpu.VMEM((GROUPS, gr, width), F32),
                pltpu.VMEM((GROUPS, gr, width), BF16), pltpu.VMEM((GROUPS, 3, block, width), BF16),
                pltpu.VMEM((GROUPS, gr, width), BF16),
                dma, dma, dma, dma((2, n_tiles)), dma((n_chunks,)), dma((2, 3)), dma((2, GROUPS, 3)), dma((2, GROUPS, 3)),
                dma((2, GROUPS, n_chunks + 1)), dma((2, n_chunks + 1)), dma((2, n_chunks)),
                dma((2, n_chunks)), dma((2, n_chunks)), dma((2, GROUPS, 3)), dma((2, GROUPS, 3))],
            compiler_params=pltpu.CompilerParams(collective_id=1, has_side_effects=True, vmem_limit_bytes=40 << 20),
        )(attn, hidden, norm_mlp, w_out, w_gate, w_up, w_down)
        shape = (rows, slots, 1, HEAD_DIM)
        return hidden_out, k_next.reshape(shape), v_next.reshape(shape)

    return jax.shard_map(local_layer, mesh=mesh, in_specs=in_specs, out_specs=out_specs, check_vma=False)
```

```python
import functools

import jax
import jax.numpy as jnp
import numpy as np
from jax import lax
from jax.experimental import pallas as pl
from jax.experimental.pallas import tpu as pltpu
from jax.sharding import PartitionSpec as P

MESH = pl.DeviceIdType.MESH
LANES = 128
HEAD_DIM = 128
ROPE_THETA = 1000000.0
NORM_EPS = 1e-6
DOWNSCALE = 2.0 ** -10
BIG = 3.3e38
GROUPS = 2
UNROLL = 8
PIECE = 512
CACHE_PARTS = 8
CHUNKS = (2, 5, 8, 8, 8, 4, 2)
EARLY = 4
SPREAD_AT = 4
F32 = jnp.float32
BF16 = jnp.bfloat16


def row_peers():
    row = lax.axis_index('row')
    core, y = row % 2, row // 2
    return row, y * 2 + 1 - core, (1 - y) * 2 + core, (1 - y) * 2 + 1 - core


def split_square(sq_sum):
    high = sq_sum.astype(BF16)
    high_f = high.astype(F32)
    low = jnp.where(high_f < BIG, sq_sum - high_f, 0.0).astype(BF16)
    return high, low


def local_scale(sq_sum, width):
    return lax.rsqrt(sq_sum / width + NORM_EPS)


def ratio(total, local):
    return jnp.where(local > 0.0, total / local, 0.0)


def remote(src, dst, send_sem, recv_sem, device):
    return pltpu.make_async_remote_copy(src_ref=src, dst_ref=dst, send_sem=send_sem, recv_sem=recv_sem,
                                        device_id=device, device_id_type=MESH)


def rotate(vec, cos_t, sin_t):
    half = HEAD_DIM // 2
    swapped = jnp.concatenate([-vec[:, half:], vec[:, :half]], axis=1)
    return (vec * cos_t + swapped * sin_t).astype(BF16).astype(F32)


def qkv_kernel(h_hbm, g_hbm, w_hbm, b_hbm, ids_hbm, freq_hbm, kc_hbm, vc_hbm, q_ref, k_ref, v_ref, kc_ref, vc_ref,
               h_ref, g_ref, w_ref, b_ref, ids_ref, freq_ref, part, send, recv, table, q_rows,
               send_sem, recv_sem, load_sem, cache_sem):
    row, *peers = row_peers()
    loads = [pltpu.make_async_copy(src, dst, load_sem.at[i]) for i, (src, dst) in enumerate(
        ((h_hbm, h_ref), (g_hbm, g_ref), (w_hbm, w_ref), (b_hbm, b_ref), (ids_hbm, ids_ref), (freq_hbm, freq_ref)))]
    for copy in loads:
        copy.start()
    width = h_ref.shape[1]
    cols = w_ref.shape[1]
    rows = k_ref.shape[0]
    group = cols // HEAD_DIM - 2
    barrier = pltpu.get_barrier_semaphore()
    for peer in peers:
        pl.semaphore_signal(barrier, inc=1, device_id={'row': peer}, device_id_type=MESH)
    cache_copies = []
    for i in range(CACHE_PARTS):
        at = pl.ds(i * (rows // CACHE_PARTS), rows // CACHE_PARTS)
        cache_copies.append(pltpu.make_async_copy(kc_hbm.at[at], kc_ref.at[at], cache_sem.at[0, i]))
        cache_copies.append(pltpu.make_async_copy(vc_hbm.at[at], vc_ref.at[at], cache_sem.at[1, i]))
    for copy in cache_copies:
        copy.start()

    loads[0].wait()
    loads[1].wait()
    hid = h_ref[...].astype(F32)
    sq_sum = jnp.sum(hid * hid, axis=1, keepdims=True)
    scale = local_scale(sq_sum, width) * DOWNSCALE
    normed = (hid * scale * g_ref[...].astype(F32).reshape(1, -1)).astype(BF16)
    loads[2].wait()
    wide = jnp.broadcast_to(sq_sum, (hid.shape[0], LANES))
    part[:, cols:] = wide
    high, low = split_square(wide)
    lane = lax.broadcasted_iota(jnp.int32, wide.shape, 1)
    send[:, 0:LANES] = jnp.where(lane < LANES // 2, high.astype(F32), low.astype(F32)).astype(BF16)
    copies = []
    for piece, (lo, hi) in enumerate(((0, PIECE), (PIECE, cols))):
        prod = jnp.dot(normed, w_ref[:, lo:hi], preferred_element_type=F32)
        part[:, lo:hi] = prod
        send[:, LANES + lo:LANES + hi] = prod.astype(BF16)
        if piece == 0:
            pl.semaphore_wait(barrier, 3)
        at = pl.ds(0, LANES + hi) if piece == 0 else pl.ds(LANES + lo, hi - lo)
        for slot in (2, 1, 0):
            copies.append(remote(send.at[pl.ds(pl.multiple_of(peers[slot] * rows, rows), rows), at], recv.at[slot, :, at],
                                 send_sem.at[piece, slot], recv_sem.at[piece, slot], {'row': peers[slot]}))
            copies[-1].start()

    for copy in loads[3:]:
        copy.wait()
    table[...] = jnp.zeros_like(table)
    table[0:3, 0:rows] = ids_ref[...].astype(F32)
    by_row = table[...].T
    pair = lax.broadcasted_iota(jnp.int32, (rows, HEAD_DIM), 1) % (HEAD_DIM // 2)
    chosen = jnp.where(pair < 16, by_row[0:rows, 0:1], jnp.where(pair < 40, by_row[0:rows, 1:2], by_row[0:rows, 2:3]))
    angles = chosen * freq_ref[...]
    cos_t, sin_t = jnp.cos(angles), jnp.sin(angles)

    for copy in copies:
        copy.wait_recv()
    mine = part[pl.ds(pl.multiple_of(row * rows, rows), rows), :]
    sums = [mine[:, cols:cols + 1]]
    parts = [mine[:, 0:cols]]
    for slot in range(3):
        block = recv[slot].astype(F32)
        sums.append(block[:, 0:1] + block[:, LANES // 2:LANES // 2 + 1])
        parts.append(block[:, LANES:])
    total = local_scale(sums[0] + sums[1] + sums[2] + sums[3], 4 * width)
    qkv = jnp.zeros((rows, cols), F32)
    for square, block in zip(sums, parts):
        qkv = qkv + block * ratio(total, local_scale(square, width) * DOWNSCALE)
    qkv = (qkv + b_ref[...].astype(F32).reshape(1, -1)).astype(BF16).astype(F32)
    for head in range(group):
        q_rows[pl.ds(head, rows, stride=8), :] = rotate(qkv[:, head * HEAD_DIM:(head + 1) * HEAD_DIM], cos_t, sin_t)
    for head in range(group, 8):
        q_rows[pl.ds(head, rows, stride=8), :] = jnp.zeros((rows, HEAD_DIM), F32)
    q_ref[...] = q_rows[...]
    k_ref[...] = rotate(qkv[:, group * HEAD_DIM:(group + 1) * HEAD_DIM], cos_t, sin_t)
    v_ref[...] = qkv[:, (group + 1) * HEAD_DIM:]
    for copy in copies:
        copy.wait_send()
    for copy in cache_copies:
        copy.wait()


def attention_kernel(group, unroll, lens_ref, q_ref, nk_ref, nv_ref, k_in, v_in, o_ref, k_out, v_out, k_ref, v_ref,
                     o_rows, s_buf, out_sem):
    rows, slots = k_ref.shape[0], k_ref.shape[1]
    steps = rows // unroll

    def stores(step):
        at = pl.ds(step * unroll, unroll)
        return (pltpu.make_async_copy(k_ref.at[at], k_out.at[at], out_sem.at[0, step]),
                pltpu.make_async_copy(v_ref.at[at], v_out.at[at], out_sem.at[1, step]))

    for step in range(steps):
        for b in range(step * unroll, (step + 1) * unroll):
            base = pl.multiple_of((lens_ref[b] // 16) * 16, 16)
            hit = lax.broadcasted_iota(jnp.int32, (16, HEAD_DIM), 0) == lens_ref[b] % 16
            for cache, new in ((k_ref, nk_ref), (v_ref, nv_ref)):
                old = cache[b, pl.ds(base, 16), :].astype(F32)
                cache[b, pl.ds(base, 16), :] = jnp.where(hit, new[b:b + 1, :], old).astype(BF16)
        if step:
            for copy in stores(step - 1):
                copy.start()
    for copy in stores(steps - 1):
        copy.start()

    @pl.loop(0, steps)
    def _(step):
        items = [step * unroll + u for u in range(unroll)]
        position = lax.broadcasted_iota(jnp.int32, (8, slots), 1)
        for u, b in enumerate(items):
            query = q_ref[pl.ds(pl.multiple_of(b * 8, 8), 8), :]
            scores = lax.dot_general(query.astype(BF16), k_ref[b], (((1,), (1,)), ((), ())),
                                     preferred_element_type=F32) * (HEAD_DIM ** -0.5)
            s_buf[u * 8:(u + 1) * 8, :] = jnp.where(position <= lens_ref[b], scores, -1e30)
        scores = s_buf[...]
        weight = jnp.exp(scores - jnp.max(scores, axis=1, keepdims=True))
        s_buf[...] = weight / jnp.sum(weight, axis=1, keepdims=True)
        for u, b in enumerate(items):
            prob = s_buf[u * 8:(u + 1) * 8, :].astype(BF16)
            o_rows[pl.ds(pl.multiple_of(b * 8, 8), 8), :] = jnp.dot(prob, v_ref[b], preferred_element_type=F32)

    for head in range(group):
        o_ref[:, head * HEAD_DIM:(head + 1) * HEAD_DIM] = o_rows[pl.ds(head, rows, stride=8), :].astype(BF16)
    for step in range(steps):
        for copy in stores(step):
            copy.wait()


def mlp_kernel(chunks, o_ref, h_hbm, g_hbm, wo_hbm, wg_hbm, wu_hbm, wd_hbm, out_ref,
               hid, g_ref, wo, wgu, wd, o_all, osend, orecv, own, resid, resid_p, z_p, sums_p, coef,
               part, send1, recv1, send2, recv2, acts, acc, dsend, drecv, final,
               h_sem, g_sem, wo_sem, wgu_sem, wd_sem, osem, rs_sem, ag_sem, s1_sem, s2_sem, ay_sem, ac_sem, aw_sem, ds_sem, da_sem):
    row, mate, across, diagonal = row_peers()
    core, y = row % 2, row // 2
    col = lax.axis_index('col')
    zpeers = [(col + step) % 4 for step in (1, 2, 3)]
    n_tiles = wgu.shape[0]
    width = hid.shape[1]
    group_rows = resid.shape[1]
    rows = group_rows // 2
    block = group_rows // 4
    base = [pl.multiple_of(y * group_rows, group_rows), pl.multiple_of((1 - y) * group_rows, group_rows)]
    n_chunks = len(chunks)
    last = n_chunks - 1

    mine = pl.ds(pl.multiple_of(core * rows, rows), rows)
    theirs = pl.ds(pl.multiple_of((1 - core) * rows, rows), rows)
    wo_copy = pltpu.make_async_copy(wo_hbm, wo, wo_sem)
    wo_copy.start()
    h_copy = pltpu.make_async_copy(h_hbm, hid, h_sem)
    h_copy.start()
    g_copy = pltpu.make_async_copy(g_hbm, g_ref, g_sem)
    g_copy.start()

    barrier = pltpu.get_barrier_semaphore()
    for peer in (diagonal, across, mate):
        pl.semaphore_signal(barrier, inc=1, device_id={'row': peer}, device_id_type=MESH)
    for peer in zpeers:
        pl.semaphore_signal(barrier, inc=1, device_id={'col': peer}, device_id_type=MESH)

    def tile_loads(t):
        at = pl.ds(pl.multiple_of(t * LANES, LANES), LANES)
        return (pltpu.make_async_copy(wg_hbm.at[:, at], wgu.at[t, :, pl.ds(0, LANES)], wgu_sem.at[0, t]),
                pltpu.make_async_copy(wu_hbm.at[:, at], wgu.at[t, :, pl.ds(LANES, LANES)], wgu_sem.at[1, t]))

    @pl.loop(0, n_tiles)
    def _(t):
        for copy in tile_loads(t):
            copy.start()

    wd_copies = []
    for k, (first, count) in enumerate(chunks):
        at = pl.ds(first * LANES, count * LANES)
        wd_copies.append(pltpu.make_async_copy(wd_hbm.at[at], wd.at[at], wd_sem.at[k]))
        wd_copies[-1].start()

    started = []

    def start(copy):
        copy.start()
        started.append(copy)
        return copy

    o_all[0, mine, :] = o_ref[...]
    pl.semaphore_wait(barrier, 6)
    gathers = [start(remote(o_ref, o_all.at[g, mine], osem.at[0, i], osem.at[1, i], {'row': peer}))
               for i, g, peer in ((0, 0, mate), (1, 1, across), (2, 1, diagonal))]

    own_rows = pl.ds(pl.multiple_of(col * block, block), block)
    scatters, spreads = {}, {}

    def project(g):
        if g == 0:
            wo_copy.wait()
            gathers[0].wait_recv()
        else:
            gathers[1].wait_recv()
            gathers[2].wait_recv()
        prod = jnp.dot(o_all[g], wo[...], preferred_element_type=F32)
        own[g] = prod
        osend[g] = prod.astype(BF16)
        scatters[g] = [start(remote(osend.at[g, pl.ds(pl.multiple_of(zpeers[i] * block, block), block)], orecv.at[g, i],
                                    rs_sem.at[0, g, i], rs_sem.at[1, g, i], {'col': zpeers[i]})) for i in (1, 2, 0)]

    def spread(g):
        if g == 0:
            h_copy.wait()
            g_copy.wait()
        for copy in scatters[g]:
            copy.wait_recv()
        total = own[g, own_rows, :]
        for i in range(3):
            total = total + orecv[g, i].astype(F32)
        old = hid[pl.ds(pl.multiple_of(base[g] + col * block, block), block), :].astype(F32)
        resid[g, own_rows, :] = (old + total).astype(BF16)
        spreads[g] = [start(remote(resid.at[g, own_rows], resid.at[g, own_rows], ag_sem.at[0, g, i], ag_sem.at[1, g, i],
                                   {'col': zpeers[i]})) for i in (1, 2, 0)]

    stage1, stage2, act_y, act_c, act_w = {}, {}, {}, {}, {}

    def norm(g):
        for copy in spreads[g]:
            copy.wait_recv()
        resid_p[g, 0:rows, :] = resid[g, mine, :]
        resid_p[g, rows:, :] = resid[g, theirs, :]
        res = resid_p[g].astype(F32)
        sq_sum = jnp.sum(res * res, axis=1, keepdims=True)
        z_p[g] = (res * (local_scale(sq_sum, width) * DOWNSCALE) * g_ref[...].astype(F32).reshape(1, -1)).astype(BF16)
        wide = jnp.broadcast_to(sq_sum, (group_rows, LANES))
        sums_p[g] = wide[0:rows]
        high, low = split_square(wide[rows:])
        send1[g, n_tiles, :, 0:LANES] = high
        send1[g, n_tiles, :, LANES:] = low
        stage1[g, n_chunks] = start(remote(send1.at[g, n_tiles], recv1.at[g, n_tiles], s1_sem.at[0, g, n_chunks],
                                           s1_sem.at[1, g, n_chunks], {'row': mate}))

    def multiply(g, k):
        first, count = chunks[k]
        if g == 0:
            @pl.loop(first, first + count)
            def _(t):
                for copy in tile_loads(t):
                    copy.wait()

        @pl.loop(first, first + count, unroll=count)
        def _(t):
            prod = jnp.dot(z_p[g], wgu[t], preferred_element_type=F32)
            part[g, t] = prod[0:rows]
            send1[g, t] = prod[rows:].astype(BF16)

        at = pl.ds(first, count)
        stage1[g, k] = start(remote(send1.at[g, at], recv1.at[g, at], s1_sem.at[0, g, k], s1_sem.at[1, g, k],
                                    {'row': mate}))

    def combine(g, k):
        first, count = chunks[k]
        if k == 0:
            stage1[g, n_chunks].wait_recv()
            got = recv1[g, n_tiles].astype(F32)
            got = got[:, 0:LANES] + got[:, LANES:]
            mine_sq = sums_p[g]
            chip_sq = mine_sq + got
            chip = local_scale(chip_sq, 2 * width)
            mine_c = ratio(chip, local_scale(mine_sq, width) * DOWNSCALE)
            mate_c = ratio(chip, local_scale(got, width) * DOWNSCALE)
            for lane in range(2):
                coef[g, 0, :, lane * LANES:(lane + 1) * LANES] = mine_c
                coef[g, 1, :, lane * LANES:(lane + 1) * LANES] = mate_c
            sums_p[g] = chip_sq
            if g == 0:
                high, low = split_square(chip_sq)
                send2[n_tiles, :, 0:LANES] = high
                send2[n_tiles, :, LANES:] = low
                stage2[n_chunks] = start(remote(send2.at[n_tiles], recv2.at[n_tiles], s2_sem.at[0, n_chunks],
                                                s2_sem.at[1, n_chunks], {'row': across}))
        stage1[g, k].wait_recv()

        @pl.loop(first, first + count, unroll=2 if count % 2 == 0 else 1)
        def _(t):
            chip = part[g, t] * coef[g, 0] + recv1[g, t].astype(F32) * coef[g, 1]
            if g == 0:
                send2[t] = chip.astype(BF16)
            else:
                part[g, t] = chip

        if g == 0:
            at = pl.ds(first, count)
            stage2[k] = start(remote(send2.at[at], recv2.at[at], s2_sem.at[0, k], s2_sem.at[1, k], {'row': across}))

    def activate(k):
        first, count = chunks[k]
        if k == 0:
            stage2[n_chunks].wait_recv()
            got = recv2[n_tiles].astype(F32)
            got = got[:, 0:LANES] + got[:, LANES:]
            chip_sq = sums_p[1]
            total = local_scale(chip_sq + got, 4 * width)
            mine_c = ratio(total, local_scale(chip_sq, 2 * width))
            other_c = ratio(total, local_scale(got, 2 * width))
            for lane in range(2):
                coef[2, 0, :, lane * LANES:(lane + 1) * LANES] = mine_c
                coef[2, 1, :, lane * LANES:(lane + 1) * LANES] = other_c
        stage2[k].wait_recv()

        @pl.loop(first, first + count, unroll=2 if count % 2 == 0 else 1)
        def _(t):
            full = part[1, t] * coef[2, 0] + recv2[t].astype(F32) * coef[2, 1]
            full = full.astype(BF16).astype(F32)
            gate, up = full[:, 0:LANES], full[:, LANES:]
            acts[1, 0:rows, pl.ds(pl.multiple_of(t * LANES, LANES), LANES)] = (
                gate * (1.0 / (1.0 + jnp.exp(-gate))) * up).astype(BF16)

        at = pl.ds(first * LANES, count * LANES)
        src = acts.at[1, pl.ds(0, rows), at]
        act_y[k] = start(remote(src, acts.at[0, pl.ds(0, rows), at], ay_sem.at[0, k], ay_sem.at[1, k], {'row': across}))
        act_c[k] = start(remote(src, acts.at[1, pl.ds(rows, rows), at], ac_sem.at[0, k], ac_sem.at[1, k], {'row': mate}))

    def relay(k):
        first, count = chunks[k]
        at = pl.ds(first * LANES, count * LANES)
        act_y[k].wait_recv()
        act_w[k] = start(remote(acts.at[0, pl.ds(0, rows), at], acts.at[0, pl.ds(rows, rows), at],
                                aw_sem.at[0, k], aw_sem.at[1, k], {'row': mate}))

    def down(g, k):
        first, count = chunks[k]
        if g == 1:
            act_c[k].wait_recv()
            wd_copies[k].wait()
        else:
            act_w[k].wait_recv()
        at = pl.ds(first * LANES, count * LANES)
        prod = jnp.dot(acts[g, :, at], wd[at, :], preferred_element_type=F32)
        acc[g] = prod if k == 0 else acc[g] + prod

    down_scatter, down_spread = {}, {}

    def scatter_down(g):
        dsend[g] = acc[g].astype(BF16)
        down_scatter[g] = [start(remote(dsend.at[g, pl.ds(pl.multiple_of(zpeers[i] * block, block), block)],
                                        drecv.at[g, i], ds_sem.at[0, g, i], ds_sem.at[1, g, i], {'col': zpeers[i]}))
                           for i in (1, 2, 0)]

    def spread_down(g):
        for copy in down_scatter[g]:
            copy.wait_recv()
        total = acc[g, own_rows, :] + resid_p[g, own_rows, :].astype(F32)
        for i in range(3):
            total = total + drecv[g, i].astype(F32)
        final[g, own_rows, :] = total.astype(BF16)
        down_spread[g] = [start(remote(final.at[g, own_rows], final.at[g, own_rows], da_sem.at[0, g, i],
                                       da_sem.at[1, g, i], {'col': zpeers[i]})) for i in (1, 2, 0)]

    def finish(g):
        for copy in down_spread[g]:
            copy.wait_recv()
        for i, half in enumerate((core, 1 - core)):
            out_ref[pl.ds(pl.multiple_of(base[g] + half * rows, rows), rows), :] = final[g, i * rows:(i + 1) * rows, :]

    plan = [(project, 0), (spread, 0), (project, 1), (norm, 0)]
    for k in range(n_chunks):
        plan += [(multiply, 0, k)] + ([(combine, 0, k - 1)] if k else [])
        if k == 1:
            plan += [(spread, 1)]
    plan += [(combine, 0, last), (norm, 1)]
    for k in range(n_chunks):
        plan += [(multiply, 1, k)] + ([(combine, 1, k - 1)] if k else [])
        if k >= EARLY:
            plan += [(activate, k - EARLY)]
    plan += [(combine, 1, last)]
    done = 0
    for k in range(n_chunks - EARLY, n_chunks):
        plan += [(activate, k)]
        while done < k:
            plan += [(down, 1, done)]
            done += 1
    plan += [(down, 1, last), (scatter_down, 1)]
    for k in range(n_chunks):
        plan += [(relay, k)] + ([(down, 0, k - 1)] if k else [])
        if k == SPREAD_AT:
            plan += [(spread_down, 1)]
    plan += [(down, 0, last), (scatter_down, 0), (finish, 1), (spread_down, 0), (finish, 0)]
    for step, *where in plan:
        step(*where)
    for copy in started:
        copy.wait_send()


def solution(mesh):
    cache_spec = P(('dp', 'row'), None, 'col', None)
    in_specs = (P('dp', 'row'), P(None, ('dp', 'row')), P(('dp', 'row')), cache_spec, cache_spec,
                P('row'), P('row', 'col'), P('col'), P('col', 'row'), P('row'),
                P('row', 'col'), P('row', 'col'), P('col', 'row'))
    out_specs = (P('dp', 'row'), cache_spec, cache_spec)
    vmem = pl.BlockSpec(memory_space=pltpu.VMEM)
    smem = pl.BlockSpec(memory_space=pltpu.SMEM)
    hbm = pl.BlockSpec(memory_space=pl.ANY)
    dma = pltpu.SemaphoreType.DMA
    pair = np.arange(HEAD_DIM) % (HEAD_DIM // 2)
    freq = (1.0 / (ROPE_THETA ** (pair.astype(np.float64) * 2.0 / HEAD_DIM))).astype(np.float32)[None, :]

    def local_layer(hidden, mrope_ids, cache_lens, k_cache, v_cache, norm_attn, w_qkv, b_qkv, w_out, norm_mlp, w_gate, w_up, w_down):
        batch, width = hidden.shape
        rows, slots, _, _ = k_cache.shape
        cols = w_qkv.shape[1]
        ff = w_gate.shape[1]
        heads = cols // HEAD_DIM - 2
        (k_flat, v_flat, hidden, w_qkv, w_out, w_gate, w_up, w_down, norm_attn, b_qkv, mrope_ids, norm_mlp, freqs) = (
            pltpu.with_memory_space_constraint(value, pltpu.HBM)
            for value in (k_cache.reshape(rows, slots, HEAD_DIM), v_cache.reshape(rows, slots, HEAD_DIM),
                          hidden, w_qkv, w_out, w_gate, w_up, w_down, norm_attn, b_qkv, mrope_ids, norm_mlp, jnp.asarray(freq)))
        cache_shape = (rows, slots, HEAD_DIM)
        query, new_key, new_val, k_near, v_near = pl.pallas_call(
            qkv_kernel, name='qkv',
            out_shape=(pltpu.VMEM((rows * 8, HEAD_DIM), F32), pltpu.VMEM((rows, HEAD_DIM), F32), pltpu.VMEM((rows, HEAD_DIM), F32),
                       pltpu.VMEM(cache_shape, BF16), pltpu.VMEM(cache_shape, BF16)),
            in_specs=[hbm] * 8, out_specs=(vmem,) * 5,
            scratch_shapes=[pltpu.VMEM((batch, width), BF16), pltpu.VMEM(norm_attn.shape, BF16), pltpu.VMEM(w_qkv.shape, BF16),
                            pltpu.VMEM(b_qkv.shape, BF16), pltpu.VMEM(mrope_ids.shape, jnp.int32), pltpu.VMEM(freq.shape, F32),
                            pltpu.VMEM((batch, cols + LANES), F32), pltpu.VMEM((batch, cols + LANES), BF16),
                            pltpu.VMEM((3, rows, cols + LANES), BF16), pltpu.VMEM((LANES, LANES), F32),
                            pltpu.VMEM((rows * 8, HEAD_DIM), F32), dma((2, 3)), dma((2, 3)), dma((6,)), dma((2, CACHE_PARTS))],
            compiler_params=pltpu.CompilerParams(collective_id=0, has_side_effects=True, vmem_limit_bytes=12 << 20),
        )(hidden, norm_attn, w_qkv, b_qkv, mrope_ids, freqs, k_flat, v_flat)

        attn, k_next, v_next, _, _ = pl.pallas_call(
            functools.partial(attention_kernel, heads, UNROLL), name='attend',
            out_shape=(pltpu.VMEM((rows, heads * HEAD_DIM), BF16),
                       jax.ShapeDtypeStruct(cache_shape, BF16), jax.ShapeDtypeStruct(cache_shape, BF16),
                       pltpu.VMEM(cache_shape, BF16), pltpu.VMEM(cache_shape, BF16)),
            in_specs=[smem, vmem, vmem, vmem, vmem, vmem], out_specs=(vmem, hbm, hbm, vmem, vmem),
            input_output_aliases={4: 3, 5: 4},
            scratch_shapes=[pltpu.VMEM((rows * 8, HEAD_DIM), F32), pltpu.VMEM((UNROLL * 8, slots), F32), dma((2, rows // UNROLL))],
            compiler_params=pltpu.CompilerParams(vmem_limit_bytes=8 << 20),
        )(cache_lens, query, new_key, new_val, k_near, v_near)

        n_tiles = ff // LANES
        chunks = [(sum(CHUNKS[:i]), count) for i, count in enumerate(CHUNKS)]
        n_chunks = len(chunks)
        gr = batch // GROUPS
        half, block = gr // 2, gr // 4
        hidden_out = pl.pallas_call(
            functools.partial(mlp_kernel, chunks), name='mlp',
            out_shape=pltpu.VMEM((batch, width), BF16),
            in_specs=[vmem] + [hbm] * 6, out_specs=vmem,
            scratch_shapes=[
                pltpu.VMEM((batch, width), BF16), pltpu.VMEM(norm_mlp.shape, BF16),
                pltpu.VMEM(w_out.shape, BF16), pltpu.VMEM((n_tiles, width, 2 * LANES), BF16), pltpu.VMEM(w_down.shape, BF16),
                pltpu.VMEM((GROUPS, gr, w_out.shape[0]), BF16), pltpu.VMEM((GROUPS, gr, width), BF16),
                pltpu.VMEM((GROUPS, 3, block, width), BF16), pltpu.VMEM((GROUPS, gr, width), F32),
                pltpu.VMEM((GROUPS, gr, width), BF16), pltpu.VMEM((GROUPS, gr, width), BF16),
                pltpu.VMEM((GROUPS, gr, width), BF16), pltpu.VMEM((GROUPS, half, LANES), F32),
                pltpu.VMEM((GROUPS + 1, 2, half, 2 * LANES), F32),
                pltpu.VMEM((GROUPS, n_tiles, half, 2 * LANES), F32),
                pltpu.VMEM((GROUPS, n_tiles + 1, half, 2 * LANES), BF16),
                pltpu.VMEM((GROUPS, n_tiles + 1, half, 2 * LANES), BF16),
                pltpu.VMEM((n_tiles + 1, half, 2 * LANES), BF16), pltpu.VMEM((n_tiles + 1, half, 2 * LANES), BF16),
                pltpu.VMEM((GROUPS, gr, ff), BF16), pltpu.VMEM((GROUPS, gr, width), F32),
                pltpu.VMEM((GROUPS, gr, width), BF16), pltpu.VMEM((GROUPS, 3, block, width), BF16),
                pltpu.VMEM((GROUPS, gr, width), BF16),
                dma, dma, dma, dma((2, n_tiles)), dma((n_chunks,)), dma((2, 3)), dma((2, GROUPS, 3)), dma((2, GROUPS, 3)),
                dma((2, GROUPS, n_chunks + 1)), dma((2, n_chunks + 1)), dma((2, n_chunks)),
                dma((2, n_chunks)), dma((2, n_chunks)), dma((2, GROUPS, 3)), dma((2, GROUPS, 3))],
            compiler_params=pltpu.CompilerParams(collective_id=1, has_side_effects=True, vmem_limit_bytes=40 << 20),
        )(attn, hidden, norm_mlp, w_out, w_gate, w_up, w_down)
        shape = (rows, slots, 1, HEAD_DIM)
        return hidden_out, k_next.reshape(shape), v_next.reshape(shape)

    return jax.shard_map(local_layer, mesh=mesh, in_specs=in_specs, out_specs=out_specs, check_vma=False)
```

```python
import functools

import jax
import jax.numpy as jnp
import numpy as np
from jax import lax
from jax.experimental import pallas as pl
from jax.experimental.pallas import tpu as pltpu
from jax.sharding import PartitionSpec as P

MESH = pl.DeviceIdType.MESH
LANES = 128
HEAD_DIM = 128
ROPE_THETA = 1000000.0
NORM_EPS = 1e-6
DOWNSCALE = 2.0 ** -10
BIG = 3.3e38
GROUPS = 2
UNROLL = 8
PIECE = 512
CACHE_PARTS = 8
CHUNKS = (4, 8, 8, 8, 6, 3)
EARLY = 3
SPREAD_AT = 3
F32 = jnp.float32
BF16 = jnp.bfloat16


def row_peers():
    row = lax.axis_index('row')
    core, y = row % 2, row // 2
    return row, y * 2 + 1 - core, (1 - y) * 2 + core, (1 - y) * 2 + 1 - core


def split_square(sq_sum):
    high = sq_sum.astype(BF16)
    high_f = high.astype(F32)
    low = jnp.where(high_f < BIG, sq_sum - high_f, 0.0).astype(BF16)
    return high, low


def local_scale(sq_sum, width):
    return lax.rsqrt(sq_sum / width + NORM_EPS)


def ratio(total, local):
    return jnp.where(local > 0.0, total / local, 0.0)


def remote(src, dst, send_sem, recv_sem, device):
    return pltpu.make_async_remote_copy(src_ref=src, dst_ref=dst, send_sem=send_sem, recv_sem=recv_sem,
                                        device_id=device, device_id_type=MESH)


def rotate(vec, cos_t, sin_t):
    half = HEAD_DIM // 2
    swapped = jnp.concatenate([-vec[:, half:], vec[:, :half]], axis=1)
    return (vec * cos_t + swapped * sin_t).astype(BF16).astype(F32)


def qkv_kernel(h_hbm, g_hbm, w_hbm, b_hbm, ids_hbm, freq_hbm, kc_hbm, vc_hbm, q_ref, k_ref, v_ref, kc_ref, vc_ref,
               h_ref, g_ref, w_ref, b_ref, ids_ref, freq_ref, part, send, recv, table, q_rows,
               send_sem, recv_sem, load_sem, cache_sem):
    row, *peers = row_peers()
    loads = [pltpu.make_async_copy(src, dst, load_sem.at[i]) for i, (src, dst) in enumerate(
        ((h_hbm, h_ref), (g_hbm, g_ref), (w_hbm, w_ref), (b_hbm, b_ref), (ids_hbm, ids_ref), (freq_hbm, freq_ref)))]
    for copy in loads:
        copy.start()
    width = h_ref.shape[1]
    cols = w_ref.shape[1]
    rows = k_ref.shape[0]
    group = cols // HEAD_DIM - 2
    barrier = pltpu.get_barrier_semaphore()
    for peer in peers:
        pl.semaphore_signal(barrier, inc=1, device_id={'row': peer}, device_id_type=MESH)
    cache_copies = []
    for i in range(CACHE_PARTS):
        at = pl.ds(i * (rows // CACHE_PARTS), rows // CACHE_PARTS)
        cache_copies.append(pltpu.make_async_copy(kc_hbm.at[at], kc_ref.at[at], cache_sem.at[0, i]))
        cache_copies.append(pltpu.make_async_copy(vc_hbm.at[at], vc_ref.at[at], cache_sem.at[1, i]))
    for copy in cache_copies:
        copy.start()

    loads[0].wait()
    loads[1].wait()
    hid = h_ref[...].astype(F32)
    sq_sum = jnp.sum(hid * hid, axis=1, keepdims=True)
    scale = local_scale(sq_sum, width) * DOWNSCALE
    normed = (hid * scale * g_ref[...].astype(F32).reshape(1, -1)).astype(BF16)
    loads[2].wait()
    wide = jnp.broadcast_to(sq_sum, (hid.shape[0], LANES))
    part[:, cols:] = wide
    high, low = split_square(wide)
    lane = lax.broadcasted_iota(jnp.int32, wide.shape, 1)
    send[:, 0:LANES] = jnp.where(lane < LANES // 2, high.astype(F32), low.astype(F32)).astype(BF16)
    copies = []
    for piece, (lo, hi) in enumerate(((0, PIECE), (PIECE, cols))):
        prod = jnp.dot(normed, w_ref[:, lo:hi], preferred_element_type=F32)
        part[:, lo:hi] = prod
        send[:, LANES + lo:LANES + hi] = prod.astype(BF16)
        if piece == 0:
            pl.semaphore_wait(barrier, 3)
        at = pl.ds(0, LANES + hi) if piece == 0 else pl.ds(LANES + lo, hi - lo)
        for slot in (2, 1, 0):
            copies.append(remote(send.at[pl.ds(pl.multiple_of(peers[slot] * rows, rows), rows), at], recv.at[slot, :, at],
                                 send_sem.at[piece, slot], recv_sem.at[piece, slot], {'row': peers[slot]}))
            copies[-1].start()

    for copy in loads[3:]:
        copy.wait()
    table[...] = jnp.zeros_like(table)
    table[0:3, 0:rows] = ids_ref[...].astype(F32)
    by_row = table[...].T
    pair = lax.broadcasted_iota(jnp.int32, (rows, HEAD_DIM), 1) % (HEAD_DIM // 2)
    chosen = jnp.where(pair < 16, by_row[0:rows, 0:1], jnp.where(pair < 40, by_row[0:rows, 1:2], by_row[0:rows, 2:3]))
    angles = chosen * freq_ref[...]
    cos_t, sin_t = jnp.cos(angles), jnp.sin(angles)

    for copy in copies:
        copy.wait_recv()
    mine = part[pl.ds(pl.multiple_of(row * rows, rows), rows), :]
    sums = [mine[:, cols:cols + 1]]
    parts = [mine[:, 0:cols]]
    for slot in range(3):
        block = recv[slot].astype(F32)
        sums.append(block[:, 0:1] + block[:, LANES // 2:LANES // 2 + 1])
        parts.append(block[:, LANES:])
    total = local_scale(sums[0] + sums[1] + sums[2] + sums[3], 4 * width)
    qkv = jnp.zeros((rows, cols), F32)
    for square, block in zip(sums, parts):
        qkv = qkv + block * ratio(total, local_scale(square, width) * DOWNSCALE)
    qkv = (qkv + b_ref[...].astype(F32).reshape(1, -1)).astype(BF16).astype(F32)
    for head in range(group):
        q_rows[pl.ds(head, rows, stride=8), :] = rotate(qkv[:, head * HEAD_DIM:(head + 1) * HEAD_DIM], cos_t, sin_t)
    for head in range(group, 8):
        q_rows[pl.ds(head, rows, stride=8), :] = jnp.zeros((rows, HEAD_DIM), F32)
    q_ref[...] = q_rows[...]
    k_ref[...] = rotate(qkv[:, group * HEAD_DIM:(group + 1) * HEAD_DIM], cos_t, sin_t)
    v_ref[...] = qkv[:, (group + 1) * HEAD_DIM:]
    for copy in copies:
        copy.wait_send()
    for copy in cache_copies:
        copy.wait()


def attention_kernel(group, unroll, lens_ref, q_ref, nk_ref, nv_ref, k_in, v_in, o_ref, k_out, v_out, k_ref, v_ref,
                     o_rows, s_buf, out_sem):
    rows, slots = k_ref.shape[0], k_ref.shape[1]
    steps = rows // unroll

    def stores(step):
        at = pl.ds(step * unroll, unroll)
        return (pltpu.make_async_copy(k_ref.at[at], k_out.at[at], out_sem.at[0, step]),
                pltpu.make_async_copy(v_ref.at[at], v_out.at[at], out_sem.at[1, step]))

    for step in range(steps):
        for b in range(step * unroll, (step + 1) * unroll):
            base = pl.multiple_of((lens_ref[b] // 16) * 16, 16)
            hit = lax.broadcasted_iota(jnp.int32, (16, HEAD_DIM), 0) == lens_ref[b] % 16
            for cache, new in ((k_ref, nk_ref), (v_ref, nv_ref)):
                old = cache[b, pl.ds(base, 16), :].astype(F32)
                cache[b, pl.ds(base, 16), :] = jnp.where(hit, new[b:b + 1, :], old).astype(BF16)
        if step:
            for copy in stores(step - 1):
                copy.start()
    for copy in stores(steps - 1):
        copy.start()

    @pl.loop(0, steps)
    def _(step):
        items = [step * unroll + u for u in range(unroll)]
        position = lax.broadcasted_iota(jnp.int32, (8, slots), 1)
        for u, b in enumerate(items):
            query = q_ref[pl.ds(pl.multiple_of(b * 8, 8), 8), :]
            scores = lax.dot_general(query.astype(BF16), k_ref[b], (((1,), (1,)), ((), ())),
                                     preferred_element_type=F32) * (HEAD_DIM ** -0.5)
            s_buf[u * 8:(u + 1) * 8, :] = jnp.where(position <= lens_ref[b], scores, -1e30)
        scores = s_buf[...]
        weight = jnp.exp(scores - jnp.max(scores, axis=1, keepdims=True))
        s_buf[...] = weight / jnp.sum(weight, axis=1, keepdims=True)
        for u, b in enumerate(items):
            prob = s_buf[u * 8:(u + 1) * 8, :].astype(BF16)
            o_rows[pl.ds(pl.multiple_of(b * 8, 8), 8), :] = jnp.dot(prob, v_ref[b], preferred_element_type=F32)

    for head in range(group):
        o_ref[:, head * HEAD_DIM:(head + 1) * HEAD_DIM] = o_rows[pl.ds(head, rows, stride=8), :].astype(BF16)
    for step in range(steps):
        for copy in stores(step):
            copy.wait()


def mlp_kernel(chunks, o_ref, h_hbm, g_hbm, wo_hbm, wg_hbm, wu_hbm, wd_hbm, out_ref,
               hid, g_ref, wo, wgu, wd, o_all, osend, orecv, own, resid, resid_p, z_p, sums_p, coef,
               part, send1, recv1, send2, recv2, acts, acc, dsend, drecv, final,
               h_sem, g_sem, wo_sem, wgu_sem, wd_sem, osem, rs_sem, ag_sem, s1_sem, s2_sem, ay_sem, ac_sem, aw_sem, ds_sem, da_sem):
    row, mate, across, diagonal = row_peers()
    core, y = row % 2, row // 2
    col = lax.axis_index('col')
    zpeers = [(col + step) % 4 for step in (1, 2, 3)]
    far = [3 - 3 * (col // 2), 2 - col // 2, col + 1 - 2 * (col % 2)]
    slots = [(peer - col + 4) % 4 - 1 for peer in far]
    n_tiles = wgu.shape[0]
    width = hid.shape[1]
    group_rows = resid.shape[1]
    rows = group_rows // 2
    block = group_rows // 4
    base = [pl.multiple_of(y * group_rows, group_rows), pl.multiple_of((1 - y) * group_rows, group_rows)]
    n_chunks = len(chunks)
    last = n_chunks - 1

    mine = pl.ds(pl.multiple_of(core * rows, rows), rows)
    theirs = pl.ds(pl.multiple_of((1 - core) * rows, rows), rows)
    wo_copy = pltpu.make_async_copy(wo_hbm, wo, wo_sem)
    wo_copy.start()
    h_copy = pltpu.make_async_copy(h_hbm, hid, h_sem)
    h_copy.start()
    g_copy = pltpu.make_async_copy(g_hbm, g_ref, g_sem)
    g_copy.start()

    barrier = pltpu.get_barrier_semaphore()
    for peer in (diagonal, across, mate):
        pl.semaphore_signal(barrier, inc=1, device_id={'row': peer}, device_id_type=MESH)
    for peer in zpeers:
        pl.semaphore_signal(barrier, inc=1, device_id={'col': peer}, device_id_type=MESH)

    def tile_loads(t):
        at = pl.ds(pl.multiple_of(t * LANES, LANES), LANES)
        return (pltpu.make_async_copy(wg_hbm.at[:, at], wgu.at[t, :, pl.ds(0, LANES)], wgu_sem.at[0, t]),
                pltpu.make_async_copy(wu_hbm.at[:, at], wgu.at[t, :, pl.ds(LANES, LANES)], wgu_sem.at[1, t]))

    @pl.loop(0, n_tiles)
    def _(t):
        for copy in tile_loads(t):
            copy.start()

    wd_copies = []
    for k, (first, count) in enumerate(chunks):
        at = pl.ds(first * LANES, count * LANES)
        wd_copies.append(pltpu.make_async_copy(wd_hbm.at[at], wd.at[at], wd_sem.at[k]))
        wd_copies[-1].start()

    started = []

    def start(copy):
        copy.start()
        started.append(copy)
        return copy

    o_all[0, mine, :] = o_ref[...]
    pl.semaphore_wait(barrier, 6)
    gathers = [start(remote(o_ref, o_all.at[g, mine], osem.at[0, i], osem.at[1, i], {'row': peer}))
               for i, g, peer in ((0, 0, mate), (1, 1, across), (2, 1, diagonal))]

    own_rows = pl.ds(pl.multiple_of(col * block, block), block)
    scatters, spreads = {}, {}

    def project(g):
        if g == 0:
            wo_copy.wait()
            gathers[0].wait_recv()
        else:
            gathers[1].wait_recv()
            gathers[2].wait_recv()
        prod = jnp.dot(o_all[g], wo[...], preferred_element_type=F32)
        own[g] = prod
        osend[g] = prod.astype(BF16)
        scatters[g] = [start(remote(osend.at[g, pl.ds(pl.multiple_of(zpeers[i] * block, block), block)], orecv.at[g, i],
                                    rs_sem.at[0, g, i], rs_sem.at[1, g, i], {'col': zpeers[i]})) for i in (1, 2, 0)]

    def spread(g):
        if g == 0:
            h_copy.wait()
            g_copy.wait()
        for copy in scatters[g]:
            copy.wait_recv()
        total = own[g, own_rows, :]
        for i in range(3):
            total = total + orecv[g, i].astype(F32)
        old = hid[pl.ds(pl.multiple_of(base[g] + col * block, block), block), :].astype(F32)
        resid[g, own_rows, :] = (old + total).astype(BF16)
        spreads[g] = [start(remote(resid.at[g, own_rows], resid.at[g, own_rows], ag_sem.at[0, g, i], ag_sem.at[1, g, i],
                                   {'col': zpeers[i]})) for i in (1, 2, 0)]

    stage1, stage2, act_y, act_c, act_w = {}, {}, {}, {}, {}

    def norm(g):
        for copy in spreads[g]:
            copy.wait_recv()
        resid_p[g, 0:rows, :] = resid[g, mine, :]
        resid_p[g, rows:, :] = resid[g, theirs, :]
        res = resid_p[g].astype(F32)
        sq_sum = jnp.sum(res * res, axis=1, keepdims=True)
        z_p[g] = (res * (local_scale(sq_sum, width) * DOWNSCALE) * g_ref[...].astype(F32).reshape(1, -1)).astype(BF16)
        wide = jnp.broadcast_to(sq_sum, (group_rows, LANES))
        sums_p[g] = wide[0:rows]
        high, low = split_square(wide[rows:])
        send1[g, n_tiles, :, 0:LANES] = high
        send1[g, n_tiles, :, LANES:] = low
        stage1[g, n_chunks] = start(remote(send1.at[g, n_tiles], recv1.at[g, n_tiles], s1_sem.at[0, g, n_chunks],
                                           s1_sem.at[1, g, n_chunks], {'row': mate}))

    def multiply(g, k):
        first, count = chunks[k]
        if g == 0:
            @pl.loop(first, first + count)
            def _(t):
                for copy in tile_loads(t):
                    copy.wait()

        @pl.loop(first, first + count, unroll=count)
        def _(t):
            prod = jnp.dot(z_p[g], wgu[t], preferred_element_type=F32)
            part[g, t] = prod[0:rows]
            send1[g, t] = prod[rows:].astype(BF16)

        at = pl.ds(first, count)
        stage1[g, k] = start(remote(send1.at[g, at], recv1.at[g, at], s1_sem.at[0, g, k], s1_sem.at[1, g, k],
                                    {'row': mate}))

    def combine(g, k):
        first, count = chunks[k]
        if k == 0:
            stage1[g, n_chunks].wait_recv()
            got = recv1[g, n_tiles].astype(F32)
            got = got[:, 0:LANES] + got[:, LANES:]
            mine_sq = sums_p[g]
            chip_sq = mine_sq + got
            chip = local_scale(chip_sq, 2 * width)
            mine_c = ratio(chip, local_scale(mine_sq, width) * DOWNSCALE)
            mate_c = ratio(chip, local_scale(got, width) * DOWNSCALE)
            for lane in range(2):
                coef[g, 0, :, lane * LANES:(lane + 1) * LANES] = mine_c
                coef[g, 1, :, lane * LANES:(lane + 1) * LANES] = mate_c
            sums_p[g] = chip_sq
            if g == 0:
                high, low = split_square(chip_sq)
                send2[n_tiles, :, 0:LANES] = high
                send2[n_tiles, :, LANES:] = low
                stage2[n_chunks] = start(remote(send2.at[n_tiles], recv2.at[n_tiles], s2_sem.at[0, n_chunks],
                                                s2_sem.at[1, n_chunks], {'row': across}))
        stage1[g, k].wait_recv()

        @pl.loop(first, first + count, unroll=2 if count % 2 == 0 else 1)
        def _(t):
            chip = part[g, t] * coef[g, 0] + recv1[g, t].astype(F32) * coef[g, 1]
            if g == 0:
                send2[t] = chip.astype(BF16)
            else:
                part[g, t] = chip

        if g == 0:
            at = pl.ds(first, count)
            stage2[k] = start(remote(send2.at[at], recv2.at[at], s2_sem.at[0, k], s2_sem.at[1, k], {'row': across}))

    def activate(k):
        first, count = chunks[k]
        if k == 0:
            stage2[n_chunks].wait_recv()
            got = recv2[n_tiles].astype(F32)
            got = got[:, 0:LANES] + got[:, LANES:]
            chip_sq = sums_p[1]
            total = local_scale(chip_sq + got, 4 * width)
            mine_c = ratio(total, local_scale(chip_sq, 2 * width))
            other_c = ratio(total, local_scale(got, 2 * width))
            for lane in range(2):
                coef[2, 0, :, lane * LANES:(lane + 1) * LANES] = mine_c
                coef[2, 1, :, lane * LANES:(lane + 1) * LANES] = other_c
        stage2[k].wait_recv()

        @pl.loop(first, first + count, unroll=2 if count % 2 == 0 else 1)
        def _(t):
            full = part[1, t] * coef[2, 0] + recv2[t].astype(F32) * coef[2, 1]
            full = full.astype(BF16).astype(F32)
            gate, up = full[:, 0:LANES], full[:, LANES:]
            acts[1, 0:rows, pl.ds(pl.multiple_of(t * LANES, LANES), LANES)] = (
                gate * (1.0 / (1.0 + jnp.exp(-gate))) * up).astype(BF16)

        at = pl.ds(first * LANES, count * LANES)
        src = acts.at[1, pl.ds(0, rows), at]
        act_y[k] = start(remote(src, acts.at[0, pl.ds(0, rows), at], ay_sem.at[0, k], ay_sem.at[1, k], {'row': across}))
        act_c[k] = start(remote(src, acts.at[1, pl.ds(rows, rows), at], ac_sem.at[0, k], ac_sem.at[1, k], {'row': mate}))

    def relay(k):
        first, count = chunks[k]
        at = pl.ds(first * LANES, count * LANES)
        act_y[k].wait_recv()
        act_w[k] = start(remote(acts.at[0, pl.ds(0, rows), at], acts.at[0, pl.ds(rows, rows), at],
                                aw_sem.at[0, k], aw_sem.at[1, k], {'row': mate}))

    def down(g, k):
        first, count = chunks[k]
        if g == 1:
            act_c[k].wait_recv()
            wd_copies[k].wait()
        else:
            act_w[k].wait_recv()
        at = pl.ds(first * LANES, count * LANES)
        prod = jnp.dot(acts[g, :, at], wd[at, :], preferred_element_type=F32)
        acc[g] = prod if k == 0 else acc[g] + prod

    down_scatter, down_spread = {}, {}

    def scatter_down(g):
        dsend[g] = acc[g].astype(BF16)
        down_scatter[g] = [start(remote(dsend.at[g, pl.ds(pl.multiple_of(far[i] * block, block), block)],
                                        drecv.at[g, slots[i]], ds_sem.at[0, g, i], ds_sem.at[1, g, slots[i]], {'col': far[i]}))
                           for i in range(3)]

    def spread_down(g):
        for copy in down_scatter[g]:
            copy.wait_recv()
        total = acc[g, own_rows, :] + resid_p[g, own_rows, :].astype(F32)
        for i in range(3):
            total = total + drecv[g, i].astype(F32)
        final[g, own_rows, :] = total.astype(BF16)
        down_spread[g] = [start(remote(final.at[g, own_rows], final.at[g, own_rows], da_sem.at[0, g, i],
                                       da_sem.at[1, g, slots[i]], {'col': far[i]})) for i in range(3)]

    def finish(g):
        for copy in down_spread[g]:
            copy.wait_recv()
        for i, half in enumerate((core, 1 - core)):
            out_ref[pl.ds(pl.multiple_of(base[g] + half * rows, rows), rows), :] = final[g, i * rows:(i + 1) * rows, :]

    plan = [(project, 0), (spread, 0), (project, 1), (norm, 0)]
    for k in range(n_chunks):
        plan += [(multiply, 0, k)] + ([(combine, 0, k - 1)] if k else [])
        if k == 2:
            plan += [(spread, 1)]
    plan += [(combine, 0, last), (norm, 1)]
    for k in range(n_chunks):
        plan += [(multiply, 1, k)] + ([(combine, 1, k - 1)] if k else [])
        if k >= EARLY:
            plan += [(activate, k - EARLY)]
    plan += [(combine, 1, last)]
    done = 0
    for k in range(n_chunks - EARLY, n_chunks):
        plan += [(activate, k)]
        while done < k:
            plan += [(down, 1, done)]
            done += 1
    plan += [(down, 1, last), (scatter_down, 1)]
    for k in range(n_chunks):
        plan += [(relay, k)] + ([(down, 0, k - 1)] if k else [])
        if k == SPREAD_AT:
            plan += [(spread_down, 1)]
    plan += [(down, 0, last), (scatter_down, 0), (finish, 1), (spread_down, 0), (finish, 0)]
    for step, *where in plan:
        step(*where)
    for copy in started:
        copy.wait_send()


def solution(mesh):
    cache_spec = P(('dp', 'row'), None, 'col', None)
    in_specs = (P('dp', 'row'), P(None, ('dp', 'row')), P(('dp', 'row')), cache_spec, cache_spec,
                P('row'), P('row', 'col'), P('col'), P('col', 'row'), P('row'),
                P('row', 'col'), P('row', 'col'), P('col', 'row'))
    out_specs = (P('dp', 'row'), cache_spec, cache_spec)
    vmem = pl.BlockSpec(memory_space=pltpu.VMEM)
    smem = pl.BlockSpec(memory_space=pltpu.SMEM)
    hbm = pl.BlockSpec(memory_space=pl.ANY)
    dma = pltpu.SemaphoreType.DMA
    pair = np.arange(HEAD_DIM) % (HEAD_DIM // 2)
    freq = (1.0 / (ROPE_THETA ** (pair.astype(np.float64) * 2.0 / HEAD_DIM))).astype(np.float32)[None, :]

    def local_layer(hidden, mrope_ids, cache_lens, k_cache, v_cache, norm_attn, w_qkv, b_qkv, w_out, norm_mlp, w_gate, w_up, w_down):
        batch, width = hidden.shape
        rows, slots, _, _ = k_cache.shape
        cols = w_qkv.shape[1]
        ff = w_gate.shape[1]
        heads = cols // HEAD_DIM - 2
        (k_flat, v_flat, hidden, w_qkv, w_out, w_gate, w_up, w_down, norm_attn, b_qkv, mrope_ids, norm_mlp, freqs) = (
            pltpu.with_memory_space_constraint(value, pltpu.HBM)
            for value in (k_cache.reshape(rows, slots, HEAD_DIM), v_cache.reshape(rows, slots, HEAD_DIM),
                          hidden, w_qkv, w_out, w_gate, w_up, w_down, norm_attn, b_qkv, mrope_ids, norm_mlp, jnp.asarray(freq)))
        cache_shape = (rows, slots, HEAD_DIM)
        query, new_key, new_val, k_near, v_near = pl.pallas_call(
            qkv_kernel, name='qkv',
            out_shape=(pltpu.VMEM((rows * 8, HEAD_DIM), F32), pltpu.VMEM((rows, HEAD_DIM), F32), pltpu.VMEM((rows, HEAD_DIM), F32),
                       pltpu.VMEM(cache_shape, BF16), pltpu.VMEM(cache_shape, BF16)),
            in_specs=[hbm] * 8, out_specs=(vmem,) * 5,
            scratch_shapes=[pltpu.VMEM((batch, width), BF16), pltpu.VMEM(norm_attn.shape, BF16), pltpu.VMEM(w_qkv.shape, BF16),
                            pltpu.VMEM(b_qkv.shape, BF16), pltpu.VMEM(mrope_ids.shape, jnp.int32), pltpu.VMEM(freq.shape, F32),
                            pltpu.VMEM((batch, cols + LANES), F32), pltpu.VMEM((batch, cols + LANES), BF16),
                            pltpu.VMEM((3, rows, cols + LANES), BF16), pltpu.VMEM((LANES, LANES), F32),
                            pltpu.VMEM((rows * 8, HEAD_DIM), F32), dma((2, 3)), dma((2, 3)), dma((6,)), dma((2, CACHE_PARTS))],
            compiler_params=pltpu.CompilerParams(collective_id=0, has_side_effects=True, vmem_limit_bytes=12 << 20),
        )(hidden, norm_attn, w_qkv, b_qkv, mrope_ids, freqs, k_flat, v_flat)

        attn, k_next, v_next, _, _ = pl.pallas_call(
            functools.partial(attention_kernel, heads, UNROLL), name='attend',
            out_shape=(pltpu.VMEM((rows, heads * HEAD_DIM), BF16),
                       jax.ShapeDtypeStruct(cache_shape, BF16), jax.ShapeDtypeStruct(cache_shape, BF16),
                       pltpu.VMEM(cache_shape, BF16), pltpu.VMEM(cache_shape, BF16)),
            in_specs=[smem, vmem, vmem, vmem, vmem, vmem], out_specs=(vmem, hbm, hbm, vmem, vmem),
            input_output_aliases={4: 3, 5: 4},
            scratch_shapes=[pltpu.VMEM((rows * 8, HEAD_DIM), F32), pltpu.VMEM((UNROLL * 8, slots), F32), dma((2, rows // UNROLL))],
            compiler_params=pltpu.CompilerParams(vmem_limit_bytes=8 << 20),
        )(cache_lens, query, new_key, new_val, k_near, v_near)

        n_tiles = ff // LANES
        chunks = [(sum(CHUNKS[:i]), count) for i, count in enumerate(CHUNKS)]
        n_chunks = len(chunks)
        gr = batch // GROUPS
        half, block = gr // 2, gr // 4
        hidden_out = pl.pallas_call(
            functools.partial(mlp_kernel, chunks), name='mlp',
            out_shape=pltpu.VMEM((batch, width), BF16),
            in_specs=[vmem] + [hbm] * 6, out_specs=vmem,
            scratch_shapes=[
                pltpu.VMEM((batch, width), BF16), pltpu.VMEM(norm_mlp.shape, BF16),
                pltpu.VMEM(w_out.shape, BF16), pltpu.VMEM((n_tiles, width, 2 * LANES), BF16), pltpu.VMEM(w_down.shape, BF16),
                pltpu.VMEM((GROUPS, gr, w_out.shape[0]), BF16), pltpu.VMEM((GROUPS, gr, width), BF16),
                pltpu.VMEM((GROUPS, 3, block, width), BF16), pltpu.VMEM((GROUPS, gr, width), F32),
                pltpu.VMEM((GROUPS, gr, width), BF16), pltpu.VMEM((GROUPS, gr, width), BF16),
                pltpu.VMEM((GROUPS, gr, width), BF16), pltpu.VMEM((GROUPS, half, LANES), F32),
                pltpu.VMEM((GROUPS + 1, 2, half, 2 * LANES), F32),
                pltpu.VMEM((GROUPS, n_tiles, half, 2 * LANES), F32),
                pltpu.VMEM((GROUPS, n_tiles + 1, half, 2 * LANES), BF16),
                pltpu.VMEM((GROUPS, n_tiles + 1, half, 2 * LANES), BF16),
                pltpu.VMEM((n_tiles + 1, half, 2 * LANES), BF16), pltpu.VMEM((n_tiles + 1, half, 2 * LANES), BF16),
                pltpu.VMEM((GROUPS, gr, ff), BF16), pltpu.VMEM((GROUPS, gr, width), F32),
                pltpu.VMEM((GROUPS, gr, width), BF16), pltpu.VMEM((GROUPS, 3, block, width), BF16),
                pltpu.VMEM((GROUPS, gr, width), BF16),
                dma, dma, dma, dma((2, n_tiles)), dma((n_chunks,)), dma((2, 3)), dma((2, GROUPS, 3)), dma((2, GROUPS, 3)),
                dma((2, GROUPS, n_chunks + 1)), dma((2, n_chunks + 1)), dma((2, n_chunks)),
                dma((2, n_chunks)), dma((2, n_chunks)), dma((2, GROUPS, 3)), dma((2, GROUPS, 3))],
            compiler_params=pltpu.CompilerParams(collective_id=1, has_side_effects=True, vmem_limit_bytes=40 << 20),
        )(attn, hidden, norm_mlp, w_out, w_gate, w_up, w_down)
        shape = (rows, slots, 1, HEAD_DIM)
        return hidden_out, k_next.reshape(shape), v_next.reshape(shape)

    return jax.shard_map(local_layer, mesh=mesh, in_specs=in_specs, out_specs=out_specs, check_vma=False)
```
